32 devices in a mesh: rep: 1 (over z), dp: 32 (over x, y, core).
Axes of the slice: x: 4, y: 4, z: 1, core: 2. Of those that a mesh axis runs over, the one named last changes fastest.
The devices are a block of a 4x4x8 slice.
Arguments:
- x: bfloat16 [32, 2048, 896], P(('rep', 'dp'))
- dy: bfloat16 [32, 2048, 896], P(('rep', 'dp'))
- w_gate: bfloat16 [2, 896, 2560], P(None, 'dp')
- w_up: bfloat16 [2, 896, 2560], P(None, 'dp')
- w_down: bfloat16 [2, 2560, 896], P(None, 'dp')
Outputs:
- output 1: bfloat16 [32, 2048, 896], P(('rep', 'dp'))
- output 2: bfloat16 [2, 896, 2560], P('rep', 'dp')
- output 3: bfloat16 [2, 896, 2560], P('rep', 'dp')
- output 4: bfloat16 [2, 2560, 896], P('rep', 'dp')
All inputs are finite; a program needn't handle non-finite values.
Results may differ from the reference program's by a relative error of at most 0.018.
Values are sent between devices in bfloat16 or wider.
A program may use at most 768 MiB of HBM per device.

```python
import jax
import jax.numpy as jnp
from jax import lax

SEQUENCES = 32
TOKENS = 2048
D = 896
FF = 2560
LAYERS = 2
NAMES = ("w_gate", "w_up", "w_down")
SHAPES = {"w_gate": (LAYERS, D, FF), "w_up": (LAYERS, D, FF), "w_down": (LAYERS, FF, D)}


def bump(key, n, height):
    away = (jnp.arange(n, dtype=jnp.int32) - jax.random.randint(key, (), 0, n, jnp.int32)) % n
    return jnp.where(away < n // 8, height, 1.0)


def together(key, own, strength):
    shared = jax.random.normal(key, own.shape[1:], jnp.float32)
    return (own + strength * shared) * lax.rsqrt(1 + strength * strength)


def setup_inputs(seed: int = 0, part: int = 0) -> dict:
    kx, kdy, ka, kb, kz, kf, kh, kl, *kw = jax.random.split(jax.random.key(seed), 8 + len(NAMES))
    kx, kdy, ka, kb = (jax.random.fold_in(k, part) for k in (kx, kdy, ka, kb))
    shape = (SEQUENCES, TOKENS, D)
    much_x, much_dy = jax.random.uniform(kz, (2,), jnp.float32, 0.0, 1.0)
    layers = 2.0 ** jax.random.uniform(kl, (LAYERS, 1, 1), jnp.float32, -1.0, 1.0)
    x = together(ka, jax.random.normal(kx, shape, jnp.float32), much_x) * bump(kf, D, 4.0)
    dy = together(kb, jax.random.normal(kdy, shape, jnp.float32), much_dy)
    drawn = {"x": x.astype(jnp.bfloat16), "dy": (dy * (SEQUENCES * TOKENS) ** -0.5).astype(jnp.bfloat16)}
    for key, name in zip(kw, NAMES, strict=True):
        w = jax.random.normal(key, SHAPES[name], jnp.float32) * SHAPES[name][1] ** -0.5
        drawn[name] = (w * {"w_gate": 1.0, "w_up": bump(kh, FF, 4.0), "w_down": layers}[name]).astype(jnp.bfloat16)
    return drawn


def matmul(a, w):
    return jnp.dot(a, w, preferred_element_type=jnp.float32).astype(jnp.bfloat16)


def normed(h):
    wide = h.astype(jnp.float32)
    scale = lax.rsqrt(jnp.mean(wide**2, -1, keepdims=True) + 1e-6)
    return (wide * scale).astype(jnp.bfloat16)


def layer(h, w):
    a = normed(h)
    gate = jnp.dot(a, w["w_gate"], preferred_element_type=jnp.float32)
    up = jnp.dot(a, w["w_up"], preferred_element_type=jnp.float32)
    return h + matmul((jax.nn.silu(gate) * up).astype(jnp.bfloat16), w["w_down"])


def stack(weights, h):
    return lax.scan(lambda h, w: (layer(h, w), None), h, weights)[0]


def reference(x, dy, w_gate, w_up, w_down):
    weights = dict(zip(NAMES, (w_gate, w_up, w_down), strict=True))

    def take(so_far, sequence):
        h, by_y = sequence
        _, back = jax.vjp(stack, weights, h)
        by_weights, by_h = back(by_y)
        return jax.tree.map(lambda total, term: total + term.astype(jnp.float32), so_far, by_weights), by_h

    none_yet = {name: jnp.zeros(w.shape, jnp.float32) for name, w in weights.items()}
    by_weights, by_x = lax.scan(take, none_yet, (x, dy))
    return (by_x, *(by_weights[name].astype(jnp.bfloat16) for name in NAMES))
```

```python
import functools
import math

import jax
import jax.numpy as jnp
from jax import lax
from jax.experimental import pallas as pl
from jax.experimental.pallas import tpu as pltpu
from jax.sharding import PartitionSpec as P

MESH = pl.DeviceIdType.MESH
F32, BF16 = jnp.float32, jnp.bfloat16


class Place:
    def __init__(self, side):
        me = lax.axis_index("dp")
        self.side = side
        self.core = me % 2
        chip = me // 2
        self.x, self.y = chip // side, chip % side
        first = self.core == 0
        self.a = jnp.where(first, self.x, self.y)
        self.b = jnp.where(first, self.y, self.x)

    def chip(self, a, b, core=None):
        first = (self.core if core is None else core) == 0
        return jnp.where(first, a * self.side + b, b * self.side + a)

    def step(self, v, by):
        return (v + by + self.side) % self.side

    def at(self, a, b):
        return {"dp": self.chip(a, b) * 2 + self.core}

    def a_next(self, by):
        return self.at(self.step(self.a, by), self.b)

    def b_next(self, by):
        return self.at(self.a, self.step(self.b, by))

    def partner(self):
        return {"dp": self.chip(self.a, self.b) * 2 + 1 - self.core}


def greet(place):
    barrier = pltpu.get_barrier_semaphore()
    peers = [place.a_next(1), place.a_next(-1), place.b_next(1), place.b_next(-1), place.partner()]
    for peer in peers:
        pl.semaphore_signal(barrier, inc=1, device_id=peer, device_id_type=MESH)
    pl.semaphore_wait(barrier, len(peers))


def halves(width):
    first = -(-width // 256) * 128
    return ((0, first), (first, width - first))


def part(place, split, ref, chip, core, half=None):
    rows, columns = ref.shape[1:]
    start, width, row, height = 0, columns, 0, rows
    if split == "columns":
        width = columns // 2
        start = core * width
    else:
        height = rows // 2
        row = pl.multiple_of(core * height, 16)
    if half is not None:
        offset, size = halves(width)[half]
        start, width = start + offset, size
    if not isinstance(start, int):
        start = pl.multiple_of(start, 128)
    return ref.at[chip, pl.ds(row, height), pl.ds(start, width)]


def block_shape(split, rows, columns):
    return (rows, columns // 2) if split == "columns" else (rows // 2, columns)


def remote(src, dst, send, recv, peer):
    copy = pltpu.make_async_remote_copy(
        src_ref=src, dst_ref=dst, send_sem=send, recv_sem=recv, device_id=peer, device_id_type=MESH
    )
    return copy


class Gather:
    COPIES = 36

    def __init__(self, place, split, own, full, send, recv):
        self.place, self.split, self.own, self.full, self.send, self.recv = place, split, own, full, send, recv

    def copy(self, slot, a, b, peer, half=None, mine=False):
        p = self.place
        chip = p.chip(a, b)
        dst = part(p, self.split, self.full, chip, p.core, half)
        src = part(p, self.split, self.own, 0, p.core, half) if mine else dst
        return remote(src, dst, self.send.at[slot], self.recv.at[slot], peer)

    def spread(self, k, a, mine=False):
        p = self.place
        base = 4 + 4 * k
        self.copy(base, a, p.b, p.b_next(1), mine=mine).start()
        self.copy(base + 1, a, p.b, p.b_next(-1), mine=mine).start()
        self.copy(20 + 4 * k, a, p.b, p.partner(), mine=mine).start()

    def keep(self, stage, sem):
        p = self.place
        into = pltpu.make_async_copy(part(p, self.split, self.own, 0, p.core), stage, sem)
        onto = pltpu.make_async_copy(stage, part(p, self.split, self.full, p.chip(p.a, p.b), p.core), sem)
        return into, onto

    def keep_in(self, stage, sem):
        self.keep(stage, sem)[0].start()

    def keep_out(self, stage, sem):
        into, onto = self.keep(stage, sem)
        into.wait()
        onto.start()

    def kept(self, stage, sem):
        self.keep(stage, sem)[1].wait()

    def first(self):
        p = self.place
        self.copy(0, p.a, p.b, p.a_next(1), mine=True).start()
        self.copy(1, p.a, p.b, p.a_next(-1), mine=True).start()
        self.spread(0, p.a, mine=True)

    def second(self):
        p = self.place
        left, right = p.step(p.a, -1), p.step(p.a, 1)
        self.copy(0, left, p.b, p.a_next(1)).wait_recv()
        self.copy(2, left, p.b, p.a_next(1), half=0).start()
        self.copy(1, right, p.b, p.a_next(1)).wait_recv()
        self.copy(3, right, p.b, p.a_next(-1), half=1).start()
        self.spread(1, left)
        self.spread(2, right)

    def third(self):
        p = self.place
        far = p.step(p.a, 2)
        self.copy(2, far, p.b, p.a_next(1), half=0).wait_recv()
        self.copy(3, far, p.b, p.a_next(1), half=1).wait_recv()
        self.spread(3, far)

    def rows(self):
        p = self.place
        return (p.a, p.step(p.a, -1), p.step(p.a, 1), p.step(p.a, 2))

    def relay(self, k):
        p = self.place
        a = self.rows()[k]
        base = 4 + 4 * k
        left, right = p.step(p.b, -1), p.step(p.b, 1)
        self.copy(base, a, left, p.b_next(1)).wait_recv()
        self.copy(base + 2, a, left, p.b_next(1), half=0).start()
        self.copy(base + 1, a, right, p.b_next(1)).wait_recv()
        self.copy(base + 3, a, right, p.b_next(-1), half=1).start()
        self.copy(20 + 4 * k + 1, a, left, p.partner()).start()
        self.copy(20 + 4 * k + 2, a, right, p.partner()).start()

    def last(self, k):
        p = self.place
        a = self.rows()[k]
        base = 4 + 4 * k
        far = p.step(p.b, 2)
        self.copy(base + 2, a, far, p.b_next(1), half=0).wait_recv()
        self.copy(base + 3, a, far, p.b_next(1), half=1).wait_recv()
        self.copy(20 + 4 * k + 3, a, far, p.partner()).start()

    def finish(self):
        p = self.place
        def wait_send(slot, like):
            remote(like, like, self.send.at[slot], self.recv.at[slot], p.a_next(1)).wait_send()

        block = part(p, self.split, self.full, 0, p.core)
        half = [part(p, self.split, self.full, 0, p.core, h) for h in (0, 1)]
        theirs = part(p, self.split, self.full, 0, 1 - p.core)
        for base in (0, 4, 8, 12, 16):
            wait_send(base, block)
            wait_send(base + 1, block)
            wait_send(base + 2, half[0])
            wait_send(base + 3, half[1])
        for slot in range(20, 36):
            wait_send(slot, block)
            remote(theirs, theirs, self.send.at[slot], self.recv.at[slot], p.partner()).wait_recv()

    def steps(self):
        return (
            [self.first, self.second, self.third]
            + [functools.partial(self.relay, k) for k in range(4)]
            + [functools.partial(self.last, k) for k in range(4)]
            + [self.finish]
        )


def woven(lists, lag):
    out = []
    longest = max(len(l) for l in lists)
    for t in range(longest + lag * (len(lists) - 1)):
        for i, l in enumerate(lists):
            if 0 <= t - lag * i < len(l):
                out.append(l[t - lag * i])
    return out


def gather_kernel(side, splits, *refs):
    n = len(splits)
    own, full, (stage, send, recv, local) = refs[:n], refs[n : 2 * n], (refs[2 * n : 3 * n], *refs[3 * n :])
    place = Place(side)
    greet(place)
    gathers = [Gather(place, s, o, f, send.at[i], recv.at[i]) for i, (s, o, f) in enumerate(zip(splits, own, full))]
    steps = [functools.partial(g.keep_in, stage[i], local.at[i]) for i, g in enumerate(gathers)]
    woven_steps = woven([g.steps() for g in gathers], 1)
    steps += woven_steps[: 2 * n]
    steps += [functools.partial(g.keep_out, stage[i], local.at[i]) for i, g in enumerate(gathers)]
    steps += woven_steps[2 * n :]
    steps += [functools.partial(g.kept, stage[i], local.at[i]) for i, g in enumerate(gathers)]
    for step in steps:
        step()


def gather(side, chips, splits, blocks, collective_id):
    n = len(splits)
    return pl.pallas_call(
        functools.partial(gather_kernel, side, splits),
        out_shape=[jax.ShapeDtypeStruct((chips, *b.shape[1:]), b.dtype) for b in blocks],
        in_specs=[pl.BlockSpec(memory_space=pl.ANY)] * n,
        out_specs=[pl.BlockSpec(memory_space=pl.ANY)] * n,
        scratch_shapes=[pltpu.VMEM(block_shape(s, *b.shape[1:]), b.dtype) for s, b in zip(splits, blocks)]
        + [
            pltpu.SemaphoreType.DMA((n, Gather.COPIES)),
            pltpu.SemaphoreType.DMA((n, Gather.COPIES)),
            pltpu.SemaphoreType.DMA((n,)),
        ],
        compiler_params=pltpu.CompilerParams(collective_id=collective_id, has_side_effects=True),
        name="gather",
    )(*blocks)


class Scatter:
    SEMS = 48

    @staticmethod
    def scratch(side, split, rows, columns):
        h, w = block_shape(split, rows, columns)
        (_, w0), (_, w1) = halves(w)
        n = side
        return [
            pltpu.VMEM((n, n, h, w), BF16),
            pltpu.VMEM((n, n, h, w), BF16),
            pltpu.VMEM((n, h, w0), BF16),
            pltpu.VMEM((n, h, w1), BF16),
            pltpu.VMEM((2, n, h, w), BF16),
            pltpu.VMEM((h, w0), BF16),
            pltpu.VMEM((h, w1), BF16),
            pltpu.VMEM((2, h, w), BF16),
        ]

    def __init__(self, place, split, terms, out, bufs, send, recv):
        self.place, self.split, self.terms, self.out, self.send, self.recv = place, split, terms, out, send, recv
        self.sums, self.theirs, self.h0, self.h1, self.full, self.g0, self.g1, self.last_in = bufs
        self.w = self.sums.shape[-1]
        (_, self.w0), (_, self.w1) = halves(self.w)

    def copies(self):
        p, n = self.place, self.place.side
        other = 1 - p.core
        for b in range(n):
            for a in range(n):
                slot = b * n + a
                mine = pltpu.make_async_copy(
                    part(p, self.split, self.terms, p.chip(a, b), p.core), self.sums.at[b, a], self.send.at[16 + slot]
                )
                sent = remote(
                    part(p, self.split, self.terms, p.chip(a, b, other), other),
                    self.theirs.at[b, a],
                    self.send.at[slot],
                    self.recv.at[slot],
                    p.partner(),
                )
                yield b, a, mine, sent

    def start(self):
        for _, _, mine, sent in self.copies():
            sent.start()
            mine.start()

    def pair(self, k):
        p = self.place
        b = p.step(p.b, k)
        for a in range(p.side):
            slot = b * p.side + a
            pltpu.make_async_copy(
                self.sums.at[b, a], self.sums.at[b, a], self.send.at[16 + slot]
            ).wait()
            remote(
                self.sums.at[b, a], self.theirs.at[b, a], self.send.at[slot], self.recv.at[slot], p.partner()
            ).wait()
            self.sums[b, a] = (self.sums[b, a].astype(F32) + self.theirs[b, a].astype(F32)).astype(BF16)

    def ring_b(self, slot, b, src, dst, by):
        return remote(src, dst, self.send.at[32 + slot], self.recv.at[32 + slot], self.place.b_next(by))

    def ring_a(self, slot, src, dst, by):
        return remote(src, dst, self.send.at[36 + slot], self.recv.at[36 + slot], self.place.a_next(by))

    def b_copies(self):
        p = self.place
        far, right, left = p.step(p.b, 2), p.step(p.b, 1), p.step(p.b, -1)
        lo, hi = pl.ds(0, self.w0), pl.ds(self.w0, self.w1)
        every = pl.ds(0, p.side)
        rows = pl.ds(0, self.sums.shape[2])
        return (
            self.ring_b(0, far, self.sums.at[far, every, rows, lo], self.h0, 1),
            self.ring_b(1, far, self.sums.at[far, every, rows, hi], self.h1, -1),
            self.ring_b(2, right, self.sums.at[right], self.full.at[0], 1),
            self.ring_b(3, left, self.sums.at[left], self.full.at[1], -1),
        )

    def b_out(self):
        c = self.b_copies()
        c[0].start()
        c[1].start()

    def b_relay(self):
        p, n = self.place, self.place.side
        c = self.b_copies()
        c[0].wait_recv()
        right, left = p.step(p.b, 1), p.step(p.b, -1)
        for a in range(n):
            self.sums[right, a, :, : self.w0] = (
                self.sums[right, a, :, : self.w0].astype(F32) + self.h0[a].astype(F32)
            ).astype(BF16)
        c[2].start()
        c[1].wait_recv()
        for a in range(n):
            self.sums[left, a, :, self.w0 :] = (
                self.sums[left, a, :, self.w0 :].astype(F32) + self.h1[a].astype(F32)
            ).astype(BF16)
        c[3].start()

    def a_copies(self):
        p = self.place
        far, right, left = p.step(p.a, 2), p.step(p.a, 1), p.step(p.a, -1)
        lo, hi = pl.ds(0, self.w0), pl.ds(self.w0, self.w1)
        rows = pl.ds(0, self.sums.shape[2])
        s = self.theirs
        return (
            self.ring_a(0, s.at[0, far, rows, lo], self.g0, 1),
            self.ring_a(1, s.at[0, far, rows, hi], self.g1, -1),
            self.ring_a(2, s.at[0, right], self.last_in.at[0], 1),
            self.ring_a(3, s.at[0, left], self.last_in.at[1], -1),
        )

    def b_in(self):
        p, n = self.place, self.place.side
        c = self.b_copies()
        c[2].wait_recv()
        c[3].wait_recv()
        for a in range(n):
            self.theirs[0, a] = (
                self.sums[p.b, a].astype(F32) + self.full[0, a].astype(F32) + self.full[1, a].astype(F32)
            ).astype(BF16)
        c = self.a_copies()
        c[0].start()
        c[1].start()

    def a_relay(self):
        p = self.place
        c = self.a_copies()
        right, left = p.step(p.a, 1), p.step(p.a, -1)
        c[0].wait_recv()
        self.theirs[0, right, :, : self.w0] = (
            self.theirs[0, right, :, : self.w0].astype(F32) + self.g0[...].astype(F32)
        ).astype(BF16)
        c[2].start()
        c[1].wait_recv()
        self.theirs[0, left, :, self.w0 :] = (
            self.theirs[0, left, :, self.w0 :].astype(F32) + self.g1[...].astype(F32)
        ).astype(BF16)
        c[3].start()

    def finish(self):
        p = self.place
        c = self.a_copies()
        c[2].wait_recv()
        c[3].wait_recv()
        self.out[...] = (
            self.theirs[0, p.a].astype(F32) + self.last_in[0].astype(F32) + self.last_in[1].astype(F32)
        ).astype(BF16)
        for copy in (*self.b_copies(), *c):
            copy.wait_send()

    def steps(self):
        return [
            self.start,
            functools.partial(self.pair, 2),
            self.b_out,
            functools.partial(self.pair, 1),
            functools.partial(self.pair, -1),
            functools.partial(self.pair, 0),
            self.b_relay,
            self.b_in,
            self.a_relay,
            self.finish,
        ]


def scatter_kernel(side, splits, *refs):
    n = len(splits)
    terms, outs, bufs, (send, recv) = refs[:n], refs[n : 2 * n], refs[2 * n : 10 * n], refs[10 * n :]
    place = Place(side)
    greet(place)
    scatters = [
        Scatter(place, splits[i], terms[i], outs[i], bufs[8 * i : 8 * i + 8], send.at[i], recv.at[i]) for i in range(n)
    ]
    lists = [s.steps() for s in scatters]
    for l in lists:
        l.pop(0)()
    for step in woven(lists, 2):
        step()


def scatter(side, splits, terms, collective_id):
    n = len(splits)
    shapes = [block_shape(s, *t.shape[1:]) for s, t in zip(splits, terms)]
    return pl.pallas_call(
        functools.partial(scatter_kernel, side, splits),
        out_shape=[jax.ShapeDtypeStruct(s, BF16) for s in shapes],
        in_specs=[pl.BlockSpec(memory_space=pl.ANY)] * n,
        out_specs=[pl.BlockSpec(memory_space=pltpu.VMEM)] * n,
        scratch_shapes=[b for s, t in zip(splits, terms) for b in Scatter.scratch(side, s, *t.shape[1:])]
        + [pltpu.SemaphoreType.DMA((n, Scatter.SEMS)), pltpu.SemaphoreType.DMA((n, Scatter.SEMS))],
        compiler_params=pltpu.CompilerParams(
            collective_id=collective_id, has_side_effects=True, vmem_limit_bytes=56 * 2**20
        ),
        name="scatter",
    )(*terms)


def dot(a, w, dims=((1,), (0,))):
    return lax.dot_general(a, w, (dims, ((), ())), preferred_element_type=F32)


def normed(h):
    wide = h.astype(F32)
    scale = lax.rsqrt(jnp.mean(wide**2, -1, keepdims=True) + 1e-6)
    return (wide * scale).astype(BF16), scale


def norm_back(h, scale, da):
    wide, ct = h.astype(F32), da.astype(F32)
    inner = jnp.sum(ct * wide, -1, keepdims=True)
    return (ct * scale - wide * (scale**3) * inner / h.shape[-1]).astype(BF16)


def solution(mesh):
    n = mesh.shape["dp"]
    chips = n // 2
    side = math.isqrt(chips)
    splits = ("columns", "columns", "rows")
    swap = [(i, i ^ 1) for i in range(n)]

    def step(x, dy, w_gate, w_up, w_down):
        x, dy = x[0], dy[0]
        layers, d_own, ff = w_gate.shape
        f_own, d = w_down.shape[1:]
        core = lax.axis_index("dp") % 2

        both = jnp.stack([w_gate, w_up])
        other = lax.ppermute(both, "dp", swap)
        both = jnp.where(core == 0, jnp.concatenate([both, other], 2), jnp.concatenate([other, both], 2))
        downs = jnp.pad(w_down, ((0, 0), (0, f_own), (0, 0)))
        downs = jnp.where(core == 0, downs, jnp.roll(downs, f_own, 1))
        weights = []
        for l in range(layers):
            full = gather(side, chips, splits, [both[0, l : l + 1], both[1, l : l + 1], downs[l : l + 1]], 1)
            weights.append([f.reshape(-1, f.shape[-1]) for f in full])

        def forward(h, w):
            a, scale = normed(h)
            gate, up = dot(a, w[0]), dot(a, w[1])
            return a, scale, gate, up, (jax.nn.silu(gate) * up).astype(BF16)

        def backward(h, saved, w, g):
            a, scale, gate, up, p = saved
            dp = dot(g, w[2], ((1,), (1,))).astype(BF16).astype(F32)
            sig = jax.nn.sigmoid(gate)
            d_up = (dp * (gate * sig)).astype(BF16)
            d_gate = (dp * up * (sig * (1 + gate * (1 - sig)))).astype(BF16)
            down = dot(p, g, ((0,), (0,))).astype(BF16)
            by_gate = dot(a, d_gate, ((0,), (0,))).astype(BF16)
            by_up = dot(a, d_up, ((0,), (0,))).astype(BF16)
            da = (
                dot(d_gate, w[0], ((1,), (1,))).astype(BF16).astype(F32)
                + dot(d_up, w[1], ((1,), (1,))).astype(BF16).astype(F32)
            ).astype(BF16)
            dh = (g.astype(F32) + norm_back(h, scale, da).astype(F32)).astype(BF16)
            terms = [t.reshape(chips, -1, t.shape[-1]) for t in (by_gate, by_up, down)]
            return dh, scatter(side, splits, terms, 2)

        hs, saved = [x], []
        for l in range(layers):
            saved.append(forward(hs[l], weights[l]))
            hs.append((hs[l].astype(F32) + dot(saved[l][4], weights[l][2]).astype(BF16).astype(F32)).astype(BF16))
        g, sums = dy, [None] * layers
        for l in reversed(range(layers)):
            g, sums[l] = backward(hs[l], saved[l], weights[l], g)
        mine = jnp.stack([jnp.stack([s[0], s[1]]) for s in sums], 1)
        lower, upper = mine[:, :, :d_own], mine[:, :, d_own:]
        got = lax.ppermute(jnp.where(core == 0, upper, lower), "dp", swap)
        by = jnp.where(core == 0, jnp.concatenate([lower, got], -1), jnp.concatenate([got, upper], -1))
        return g[None], by[0], by[1], jnp.stack([s[2] for s in sums])

    wspec = P(None, "dp", None)
    out = P("rep", "dp", None)
    rows = P(("rep", "dp"), None, None)
    return jax.shard_map(
        step, mesh=mesh, in_specs=(rows, rows, wspec, wspec, wspec), out_specs=(rows, out, out, out), check_vma=False
    )
```

```python
import functools
import math

import jax
import jax.numpy as jnp
from jax import lax
from jax.experimental import pallas as pl
from jax.experimental.pallas import tpu as pltpu
from jax.sharding import PartitionSpec as P

MESH = pl.DeviceIdType.MESH
F32, BF16 = jnp.float32, jnp.bfloat16


class Place:
    def __init__(self, side):
        me = lax.axis_index("dp")
        self.side = side
        self.core = me % 2
        chip = me // 2
        self.x, self.y = chip // side, chip % side
        first = self.core == 0
        self.a = jnp.where(first, self.x, self.y)
        self.b = jnp.where(first, self.y, self.x)

    def chip(self, a, b, core=None):
        first = (self.core if core is None else core) == 0
        return jnp.where(first, a * self.side + b, b * self.side + a)

    def step(self, v, by):
        return (v + by + self.side) % self.side

    def at(self, a, b):
        return {"dp": self.chip(a, b) * 2 + self.core}

    def a_next(self, by):
        return self.at(self.step(self.a, by), self.b)

    def b_next(self, by):
        return self.at(self.a, self.step(self.b, by))

    def partner(self):
        return {"dp": self.chip(self.a, self.b) * 2 + 1 - self.core}


def greet(place):
    barrier = pltpu.get_barrier_semaphore()
    peers = [place.a_next(1), place.a_next(-1), place.b_next(1), place.b_next(-1), place.partner()]
    for peer in peers:
        pl.semaphore_signal(barrier, inc=1, device_id=peer, device_id_type=MESH)
    pl.semaphore_wait(barrier, len(peers))


def halves(width):
    first = -(-width // 256) * 128
    return ((0, first), (first, width - first))


def part(place, split, ref, chip, core, half=None):
    rows, columns = ref.shape[1:]
    start, width, row, height = 0, columns, 0, rows
    if split == "columns":
        width = columns // 2
        start = core * width
    else:
        height = rows // 2
        row = pl.multiple_of(core * height, 16)
    if half is not None:
        offset, size = halves(width)[half]
        start, width = start + offset, size
    if not isinstance(start, int):
        start = pl.multiple_of(start, 128)
    return ref.at[chip, pl.ds(row, height), pl.ds(start, width)]


def block_shape(split, rows, columns):
    return (rows, columns // 2) if split == "columns" else (rows // 2, columns)


def remote(src, dst, send, recv, peer):
    copy = pltpu.make_async_remote_copy(
        src_ref=src, dst_ref=dst, send_sem=send, recv_sem=recv, device_id=peer, device_id_type=MESH
    )
    return copy


class Gather:
    COPIES = 36

    def __init__(self, place, split, own, full, send, recv):
        self.place, self.split, self.own, self.full, self.send, self.recv = place, split, own, full, send, recv

    def copy(self, slot, a, b, peer, half=None, mine=False):
        p = self.place
        chip = p.chip(a, b)
        dst = part(p, self.split, self.full, chip, p.core, half)
        src = part(p, self.split, self.own, 0, p.core, half) if mine else dst
        return remote(src, dst, self.send.at[slot], self.recv.at[slot], peer)

    def spread(self, k, a, mine=False):
        p = self.place
        base = 4 + 4 * k
        self.copy(base, a, p.b, p.b_next(1), mine=mine).start()
        self.copy(base + 1, a, p.b, p.b_next(-1), mine=mine).start()
        self.copy(20 + 4 * k, a, p.b, p.partner(), mine=mine).start()

    def keep(self, stage, sem):
        p = self.place
        into = pltpu.make_async_copy(part(p, self.split, self.own, 0, p.core), stage, sem)
        onto = pltpu.make_async_copy(stage, part(p, self.split, self.full, p.chip(p.a, p.b), p.core), sem)
        return into, onto

    def keep_in(self, stage, sem):
        self.keep(stage, sem)[0].start()

    def keep_out(self, stage, sem):
        into, onto = self.keep(stage, sem)
        into.wait()
        onto.start()

    def kept(self, stage, sem):
        self.keep(stage, sem)[1].wait()

    def first(self):
        p = self.place
        self.copy(0, p.a, p.b, p.a_next(1), mine=True).start()
        self.copy(1, p.a, p.b, p.a_next(-1), mine=True).start()
        self.spread(0, p.a, mine=True)

    def second(self):
        p = self.place
        left, right = p.step(p.a, -1), p.step(p.a, 1)
        self.copy(0, left, p.b, p.a_next(1)).wait_recv()
        self.copy(2, left, p.b, p.a_next(1), half=0).start()
        self.copy(1, right, p.b, p.a_next(1)).wait_recv()
        self.copy(3, right, p.b, p.a_next(-1), half=1).start()
        self.spread(1, left)
        self.spread(2, right)

    def third(self):
        p = self.place
        far = p.step(p.a, 2)
        self.copy(2, far, p.b, p.a_next(1), half=0).wait_recv()
        self.copy(3, far, p.b, p.a_next(1), half=1).wait_recv()
        self.spread(3, far)

    def rows(self):
        p = self.place
        return (p.a, p.step(p.a, -1), p.step(p.a, 1), p.step(p.a, 2))

    def relay(self, k):
        p = self.place
        a = self.rows()[k]
        base = 4 + 4 * k
        left, right = p.step(p.b, -1), p.step(p.b, 1)
        self.copy(base, a, left, p.b_next(1)).wait_recv()
        self.copy(base + 2, a, left, p.b_next(1), half=0).start()
        self.copy(base + 1, a, right, p.b_next(1)).wait_recv()
        self.copy(base + 3, a, right, p.b_next(-1), half=1).start()
        self.copy(20 + 4 * k + 1, a, left, p.partner()).start()
        self.copy(20 + 4 * k + 2, a, right, p.partner()).start()

    def last(self, k):
        p = self.place
        a = self.rows()[k]
        base = 4 + 4 * k
        far = p.step(p.b, 2)
        self.copy(base + 2, a, far, p.b_next(1), half=0).wait_recv()
        self.copy(base + 3, a, far, p.b_next(1), half=1).wait_recv()
        self.copy(20 + 4 * k + 3, a, far, p.partner()).start()

    def finish(self):
        p = self.place
        def wait_send(slot, like):
            remote(like, like, self.send.at[slot], self.recv.at[slot], p.a_next(1)).wait_send()

        block = part(p, self.split, self.full, 0, p.core)
        half = [part(p, self.split, self.full, 0, p.core, h) for h in (0, 1)]
        theirs = part(p, self.split, self.full, 0, 1 - p.core)
        def ring(i, _):
            base = 4 * i
            wait_send(base, block)
            wait_send(base + 1, block)
            wait_send(base + 2, half[0])
            wait_send(base + 3, half[1])
            return 0

        def across(slot, _):
            wait_send(slot, block)
            remote(theirs, theirs, self.send.at[slot], self.recv.at[slot], p.partner()).wait_recv()
            return 0

        lax.fori_loop(0, 5, ring, 0)
        lax.fori_loop(20, 36, across, 0)

    def timed(self, i, stage, sem):
        relay = [functools.partial(self.relay, k) for k in range(4)]
        last = [functools.partial(self.last, k) for k in range(4)]
        return [
            (0, functools.partial(self.keep_in, stage, sem)),
            (0, self.first),
            (1, functools.partial(self.keep_out, stage, sem)),
            (3 + i, self.second),
            (6 + i, relay[0]),
            (7 + i, self.third),
            (9 + i, relay[1]),
            (11 + i, relay[2]),
            (13 + i, last[0]),
            (14 + i, relay[3]),
            (16 + i, last[1]),
            (18 + i, last[2]),
            (20 + i, last[3]),
            (23, self.finish),
            (23, functools.partial(self.kept, stage, sem)),
        ]


def gather_kernel(side, splits, *refs):
    n = len(splits)
    own, full, (stage, send, recv, local) = refs[:n], refs[n : 2 * n], (refs[2 * n : 3 * n], *refs[3 * n :])
    place = Place(side)
    greet(place)
    for _, event in sorted(gather_events(place, splits, own, full, stage, send, recv, local), key=lambda e: e[0]):
        event()


def gather(side, chips, splits, blocks, collective_id):
    n = len(splits)
    return pl.pallas_call(
        functools.partial(gather_kernel, side, splits),
        out_shape=[jax.ShapeDtypeStruct((chips, *b.shape[1:]), b.dtype) for b in blocks],
        in_specs=[pl.BlockSpec(memory_space=pl.ANY)] * n,
        out_specs=[pl.BlockSpec(memory_space=pl.ANY)] * n,
        scratch_shapes=[pltpu.VMEM(block_shape(s, *b.shape[1:]), b.dtype) for s, b in zip(splits, blocks)]
        + [
            pltpu.SemaphoreType.DMA((n, Gather.COPIES)),
            pltpu.SemaphoreType.DMA((n, Gather.COPIES)),
            pltpu.SemaphoreType.DMA((n,)),
        ],
        compiler_params=pltpu.CompilerParams(collective_id=collective_id, has_side_effects=True),
        name="gather",
    )(*blocks)


class Scatter:
    SEMS = 48

    @staticmethod
    def scratch(side, split, rows, columns):
        h, w = block_shape(split, rows, columns)
        (_, w0), (_, w1) = halves(w)
        n = side
        return [
            pltpu.VMEM((n, n, h, w), BF16),
            pltpu.VMEM((n, n, h, w), BF16),
            pltpu.VMEM((n, h, w0), BF16),
            pltpu.VMEM((n, h, w1), BF16),
            pltpu.VMEM((2, n, h, w), BF16),
            pltpu.VMEM((h, w0), BF16),
            pltpu.VMEM((h, w1), BF16),
            pltpu.VMEM((2, h, w), BF16),
        ]

    def __init__(self, place, split, terms, out, bufs, send, recv, near=False):
        self.near = near
        self.place, self.split, self.terms, self.out, self.send, self.recv = place, split, terms, out, send, recv
        self.sums, self.theirs, self.h0, self.h1, self.full, self.g0, self.g1, self.last_in = bufs
        self.w = self.sums.shape[-1]
        (_, self.w0), (_, self.w1) = halves(self.w)

    def start(self):
        p, n = self.place, self.place.side
        other = 1 - p.core
        for k in (2, 1, -1, 0):

            def send(a, _, k=k):
                b = p.step(p.a, k)
                slot = b * n + a
                remote(
                    part(p, self.split, self.terms, p.chip(a, b, other), other),
                    self.theirs.at[b, a],
                    self.send.at[slot],
                    self.recv.at[slot],
                    p.partner(),
                ).start()
                if not self.near:
                    b = p.step(p.b, k)
                    pltpu.make_async_copy(
                        part(p, self.split, self.terms, p.chip(a, b), p.core),
                        self.sums.at[b, a],
                        self.send.at[16 + b * n + a],
                    ).start()
                return 0

            lax.fori_loop(0, n, send, 0)

    def pair(self, k):
        p = self.place
        b = p.step(p.b, k)

        def add(a, _):
            slot = b * p.side + a
            mine = self.sums.at[b, a]
            if self.near:
                mine = part(p, self.split, self.terms, p.chip(a, b), p.core)
            else:
                pltpu.make_async_copy(mine, mine, self.send.at[16 + slot]).wait()
            remote(
                self.sums.at[b, a], self.theirs.at[b, a], self.send.at[slot], self.recv.at[slot], p.partner()
            ).wait_recv()
            self.sums[b, a] = (mine[...].astype(F32) + self.theirs[b, a].astype(F32)).astype(BF16)
            return 0

        lax.fori_loop(0, p.side, add, 0)

    def ring_b(self, slot, b, src, dst, by):
        return remote(src, dst, self.send.at[32 + slot], self.recv.at[32 + slot], self.place.b_next(by))

    def ring_a(self, slot, src, dst, by):
        return remote(src, dst, self.send.at[36 + slot], self.recv.at[36 + slot], self.place.a_next(by))

    def b_copies(self):
        p = self.place
        far, right, left = p.step(p.b, 2), p.step(p.b, 1), p.step(p.b, -1)
        lo, hi = pl.ds(0, self.w0), pl.ds(self.w0, self.w1)
        every = pl.ds(0, p.side)
        rows = pl.ds(0, self.sums.shape[2])
        return (
            self.ring_b(0, far, self.sums.at[far, every, rows, lo], self.h0, 1),
            self.ring_b(1, far, self.sums.at[far, every, rows, hi], self.h1, -1),
            self.ring_b(2, right, self.sums.at[right], self.full.at[0], 1),
            self.ring_b(3, left, self.sums.at[left], self.full.at[1], -1),
        )

    def b_out(self):
        c = self.b_copies()
        c[0].start()
        c[1].start()

    def b_relay(self):
        p, n = self.place, self.place.side
        c = self.b_copies()
        c[0].wait_recv()
        right, left = p.step(p.b, 1), p.step(p.b, -1)

        def add_low(a, _):
            self.sums[right, a, :, : self.w0] = (
                self.sums[right, a, :, : self.w0].astype(F32) + self.h0[a].astype(F32)
            ).astype(BF16)
            return 0

        def add_high(a, _):
            self.sums[left, a, :, self.w0 :] = (
                self.sums[left, a, :, self.w0 :].astype(F32) + self.h1[a].astype(F32)
            ).astype(BF16)
            return 0

        lax.fori_loop(0, n, add_low, 0)
        c[2].start()
        c[1].wait_recv()
        lax.fori_loop(0, n, add_high, 0)
        c[3].start()

    def a_copies(self):
        p = self.place
        far, right, left = p.step(p.a, 2), p.step(p.a, 1), p.step(p.a, -1)
        lo, hi = pl.ds(0, self.w0), pl.ds(self.w0, self.w1)
        rows = pl.ds(0, self.sums.shape[2])
        s = self.theirs
        return (
            self.ring_a(0, s.at[0, far, rows, lo], self.g0, 1),
            self.ring_a(1, s.at[0, far, rows, hi], self.g1, -1),
            self.ring_a(2, s.at[0, right], self.last_in.at[0], 1),
            self.ring_a(3, s.at[0, left], self.last_in.at[1], -1),
        )

    def b_in(self):
        p, n = self.place, self.place.side
        c = self.b_copies()
        c[2].wait_recv()
        c[3].wait_recv()

        def add(a, _):
            self.theirs[0, a] = (
                self.sums[p.b, a].astype(F32) + self.full[0, a].astype(F32) + self.full[1, a].astype(F32)
            ).astype(BF16)
            return 0

        lax.fori_loop(0, n, add, 0)
        c = self.a_copies()
        c[0].start()
        c[1].start()

    def a_relay(self):
        p = self.place
        c = self.a_copies()
        right, left = p.step(p.a, 1), p.step(p.a, -1)
        c[0].wait_recv()
        self.theirs[0, right, :, : self.w0] = (
            self.theirs[0, right, :, : self.w0].astype(F32) + self.g0[...].astype(F32)
        ).astype(BF16)
        c[2].start()
        c[1].wait_recv()
        self.theirs[0, left, :, self.w0 :] = (
            self.theirs[0, left, :, self.w0 :].astype(F32) + self.g1[...].astype(F32)
        ).astype(BF16)
        c[3].start()

    def finish(self):
        p = self.place
        c = self.a_copies()
        c[2].wait_recv()
        c[3].wait_recv()
        self.out[...] = (
            self.theirs[0, p.a].astype(F32) + self.last_in[0].astype(F32) + self.last_in[1].astype(F32)
        ).astype(BF16)
        for copy in (*self.b_copies(), *c):
            copy.wait_send()

        def sent(slot, _):
            first = self.theirs.at[0, 0]
            remote(self.sums.at[0, 0], first, self.send.at[slot], self.recv.at[slot], p.partner()).wait_send()
            return 0

        lax.fori_loop(0, p.side * p.side, sent, 0)

    def timed(self, base, times):
        steps = (
            self.start,
            functools.partial(self.pair, 2),
            self.b_out,
            functools.partial(self.pair, 1),
            functools.partial(self.pair, -1),
            functools.partial(self.pair, 0),
            self.b_relay,
            self.b_in,
            self.a_relay,
            self.finish,
        )
        return [(base + t, s) for t, s in zip(times, steps)]


TILE, CHUNK, SUB = 512, 512, 256
BIG, PART = 1024, 512


def scaled(h):
    wide = h.astype(F32)
    return wide, lax.rsqrt(jnp.mean(wide**2, -1, keepdims=True) + 1e-6)


def normed(h):
    wide, scale = scaled(h)
    return (wide * scale).astype(BF16)


def state_back(h, g, da):
    wide, scale = scaled(h)
    ct = da.astype(F32)
    inner = jnp.sum(ct * wide, -1, keepdims=True)
    by_h = (ct * scale - wide * (scale**3) * inner / h.shape[-1]).astype(BF16)
    return (g.astype(F32) + by_h.astype(F32)).astype(BF16)


def parts_of(t, tile, sub):
    return [pl.ds(pl.multiple_of(t * tile + i * sub, sub), sub) for i in range(tile // sub)]


ANY = pl.BlockSpec(memory_space=pl.ANY)


def dot(a, w, dims=((1,), (0,))):
    return lax.dot_general(a, w, (dims, ((), ())), preferred_element_type=F32)


def run_at(slot, slots, events, span=None):
    span = span or slots
    events = [(min(t * slots // span, slots - 1), e) for t, e in sorted(events, key=lambda e: e[0])]
    for s in sorted({t for t, _ in events}):

        @pl.when(slot == s)
        def _(s=s):
            for t, event in events:
                if t == s:
                    event()


def gather_events(place, splits, own, full, stage, send, recv, local):
    events = []
    for i, (split, o, f) in enumerate(zip(splits, own, full)):
        events += Gather(place, split, o, f, send.at[i], recv.at[i]).timed(i, stage[i], local.at[i])
    return events


def gather_scratch(splits, blocks):
    n = len(splits)
    return [pltpu.VMEM(block_shape(s, *b.shape[1:]), b.dtype) for s, b in zip(splits, blocks)] + [
        pltpu.SemaphoreType.DMA((n, Gather.COPIES)),
        pltpu.SemaphoreType.DMA((n, Gather.COPIES)),
        pltpu.SemaphoreType.DMA((n,)),
    ]


def forward_kernel(side, splits, chunks, tiles, x_ref, wg_ref, wu_ref, wd_ref, *refs):
    n = len(splits)
    own, (h_ref, gate_ref, up_ref, at_ref), refs = refs[:n], refs[n : n + 4], refs[n + 4 :]
    full, (p_ref, a_ref), stage, (send, recv, local) = refs[:n], refs[n : n + 2], refs[n + 2 : 2 * n + 2], refs[2 * n + 2 :]
    place = Place(side)
    c, t = pl.program_id(0), pl.program_id(1)
    events = [(0, functools.partial(greet, place))] + gather_events(place, splits, own, full, stage, send, recv, local)
    run_at(c * tiles + t, (chunks + 1) * tiles, events, 24)
    rows = pl.ds(pl.multiple_of(t * TILE, TILE), TILE)

    @pl.when(c == 0)
    def _():
        a = normed(x_ref[rows, :])
        a_ref[rows, :] = a
        at_ref[...] = a.T

    @pl.when(c < chunks)
    def _():
        columns = pl.ds(pl.multiple_of(c * CHUNK, CHUNK), CHUNK)
        for i, part_rows in enumerate(parts_of(t, TILE, SUB)):
            a = a_ref[part_rows, :]
            gate = dot(a, wg_ref[...])
            up = dot(a, wu_ref[...])
            gate_ref[i * SUB : (i + 1) * SUB, :] = gate
            up_ref[i * SUB : (i + 1) * SUB, :] = up
            p_ref[part_rows, columns] = (gate * jax.nn.sigmoid(gate) * up).astype(BF16)

    @pl.when(c == chunks)
    def _():
        down = dot(p_ref[rows, :], wd_ref[...]).astype(BF16)
        h_ref[...] = (x_ref[rows, :].astype(F32) + down.astype(F32)).astype(BF16)


def forward(side, chips, splits, x, weights, blocks, collective_id):
    tokens, d = x.shape
    ff = weights[0].shape[1]
    n, chunks, tiles = len(splits), ff // CHUNK, tokens // TILE
    last = chunks - 1
    wide = pl.BlockSpec((d, CHUNK), lambda c, t: (0, jnp.minimum(c, last)))
    tile = pl.BlockSpec((TILE, d), lambda c, t: (jnp.where(c == chunks, t, 0), 0))
    kept = pl.BlockSpec((TILE, CHUNK), lambda c, t: (jnp.where(c == chunks, tiles - 1, t), jnp.minimum(c, last)))
    turned = pl.BlockSpec((d, TILE), lambda c, t: (0, jnp.where(c == 0, t, tiles - 1)))
    out = pl.pallas_call(
        functools.partial(forward_kernel, side, splits, chunks, tiles),
        grid=(chunks + 1, tiles),
        out_shape=[
            jax.ShapeDtypeStruct(x.shape, BF16),
            jax.ShapeDtypeStruct((tokens, ff), F32),
            jax.ShapeDtypeStruct((tokens, ff), F32),
            jax.ShapeDtypeStruct((d, tokens), BF16),
        ]
        + [jax.ShapeDtypeStruct((chips, *b.shape[1:]), b.dtype) for b in blocks],
        in_specs=[
            pl.BlockSpec((tokens, d), lambda c, t: (0, 0), pipeline_mode=pl.Buffered(1)),
            wide,
            wide,
            pl.BlockSpec((ff, d), lambda c, t: (0, 0), pipeline_mode=pl.Buffered(1)),
        ]
        + [ANY] * n,
        out_specs=[tile, kept, kept, turned] + [ANY] * n,
        scratch_shapes=[pltpu.VMEM((tokens, ff), BF16), pltpu.VMEM((tokens, d), BF16)] + gather_scratch(splits, blocks),
        compiler_params=pltpu.CompilerParams(
            collective_id=collective_id, has_side_effects=True, vmem_limit_bytes=60 * 2**20,
            dimension_semantics=("arbitrary", "arbitrary"),
        ),
        name="forward",
    )(x, *weights, *blocks)
    return out[0], out[1:4], out[4:]


def top_kernel(chunks, tiles, h_ref, g_ref, wg_ref, wu_ref, wd_ref, *refs):
    by_gate, by_up, by_down, da_ref, acc, p_ref, dg_ref, du_ref, da_stage, at_ref, a_ref, da_sem = refs
    c, t = pl.program_id(0), pl.program_id(1)

    rows = pl.ds(pl.multiple_of(t * BIG, BIG), BIG)

    @pl.when((t < tiles) & (c == 0))
    def _():
        a = normed(h_ref[rows, :])
        a_ref[rows, :] = a
        at_ref[:, rows] = a.T

    @pl.when(t < tiles)
    def _():
        def some(i, _):
            r = pl.ds(pl.multiple_of(t * BIG + i * PART, PART), PART)
            a, g = a_ref[r, :], g_ref[r, :]
            gate, up, dp = dot(a, wg_ref[...]), dot(a, wu_ref[...]), d_hidden(g, wd_ref)
            p_ref[r, :], dg_ref[r, :], du_ref[r, :] = add_da(c, r, gate, up, dp, wg_ref, wu_ref, acc)
            return 0

        lax.fori_loop(0, BIG // PART, some, 0)

    @pl.when((t < tiles) & (c == chunks - 1))
    def _():
        da_stage[rows, :] = state_back(h_ref[rows, :], g_ref[rows, :], acc[rows, :].astype(BF16))

    @pl.when(t == tiles)
    def _():
        by_down[...] = dot(p_ref[...], g_ref[...], ((0,), (0,))).astype(BF16)

    @pl.when(t == tiles + 1)
    def _():
        by_gate[...] = dot(at_ref[...], dg_ref[...]).astype(BF16)

    @pl.when(t == tiles + 2)
    def _():
        by_up[...] = dot(at_ref[...], du_ref[...]).astype(BF16)

        @pl.when(c == chunks - 1)
        def _():
            copy = pltpu.make_async_copy(da_stage, da_ref, da_sem)
            copy.start()
            copy.wait()


def d_hidden(g, wd_ref):
    return dot(g, wd_ref[...], ((1,), (1,))).astype(BF16).astype(F32)


def add_da(c, rows, gate, up, dp, wg_ref, wu_ref, acc):
    sig = jax.nn.sigmoid(gate)
    act = gate * sig
    d_gate = (dp * up * (sig * (1 + gate * (1 - sig)))).astype(BF16)
    d_up = (dp * act).astype(BF16)
    da = dot(d_gate, wg_ref[...], ((1,), (1,))) + dot(d_up, wu_ref[...], ((1,), (1,)))
    acc[rows, :] = jnp.where(c == 0, 0.0, acc[rows, :]) + da
    return (act * up).astype(BF16), d_gate, d_up


def top(h, g, weights):
    tokens, d = h.shape
    ff = weights[0].shape[1]
    chunks, tiles = ff // CHUNK, tokens // BIG
    whole = pl.BlockSpec((tokens, d), lambda c, t: (0, 0), pipeline_mode=pl.Buffered(1))
    wide = pl.BlockSpec((d, CHUNK), lambda c, t: (0, c))
    tall = pl.BlockSpec((CHUNK, d), lambda c, t: (c, 0))
    shape = jax.ShapeDtypeStruct
    out = pl.pallas_call(
        functools.partial(top_kernel, chunks, tiles),
        grid=(chunks, tiles + 3),
        out_shape=[shape((d, ff), BF16), shape((d, ff), BF16), shape((ff, d), BF16), shape((tokens, d), BF16)],
        in_specs=[whole, whole, wide, wide, tall],
        out_specs=[wide, wide, tall, ANY],
        scratch_shapes=[pltpu.VMEM((tokens, d), F32)]
        + [pltpu.VMEM((tokens, CHUNK), BF16)] * 3
        + [pltpu.VMEM((tokens, d), BF16), pltpu.VMEM((d, tokens), BF16)]
        + [pltpu.VMEM((tokens, d), BF16), pltpu.SemaphoreType.DMA(())],
        compiler_params=pltpu.CompilerParams(
            vmem_limit_bytes=60 * 2**20, dimension_semantics=("arbitrary", "arbitrary")
        ),
        name="top",
    )(h, g, *weights)
    return out[:3], out[3]


def lower_kernel(side, splits, chunks, tiles, h_ref, g_ref, gate_ref, up_ref, wg_ref, wu_ref, wd_ref, *refs):
    n = len(splits)
    terms, (by_down, da_ref, dg_ref, du_ref), refs = refs[:n], refs[n : n + 4], refs[n + 4 :]
    outs, (acc, p_ref, da_stage, da_sem), refs = refs[:n], refs[n : n + 4], refs[n + 4 :]
    bufs, (send, recv) = refs[: 8 * n], refs[8 * n :]
    c, t = pl.program_id(0), pl.program_id(1)
    place = Place(side)
    events = [(0, functools.partial(greet, place))]
    for i in range(n):
        s = Scatter(place, splits[i], terms[i], outs[i], bufs[8 * i : 8 * i + 8], send.at[i], recv.at[i])
        events += s.timed(0, [0] + [4 * i + k for k in (2, 2, 3, 3, 4, 6, 10, 12, 14)])
    run_at(c * (tiles + 1) + t, chunks * (tiles + 1), events)

    rows = pl.ds(pl.multiple_of(t * TILE, TILE), TILE)

    @pl.when(t < tiles)
    def _():
        parts = parts_of(t, TILE, SUB)
        dps = [d_hidden(g_ref[r, :], wd_ref) for r in parts]
        for i, (r, dp) in enumerate(zip(parts, dps)):
            here = slice(i * SUB, (i + 1) * SUB)
            p_ref[r, :], dg_ref[here, :], du_ref[here, :] = add_da(
                c, r, gate_ref[here, :], up_ref[here, :], dp, wg_ref, wu_ref, acc
            )

    @pl.when((t < tiles) & (c == chunks - 1))
    def _():
        da_stage[rows, :] = state_back(h_ref[rows, :], g_ref[rows, :], acc[rows, :].astype(BF16))

    @pl.when(t == tiles)
    def _():
        by_down[...] = dot(p_ref[...], g_ref[...], ((0,), (0,))).astype(BF16)

        @pl.when(c == chunks - 1)
        def _():
            copy = pltpu.make_async_copy(da_stage, da_ref, da_sem)
            copy.start()
            copy.wait()


def lower(side, splits, kept, h, g, weights, terms, collective_id):
    tokens, d = g.shape
    ff = weights[0].shape[1]
    n, chunks, tiles = len(terms), ff // CHUNK, tokens // TILE
    whole = pl.BlockSpec((tokens, d), lambda c, t: (0, 0), pipeline_mode=pl.Buffered(1))
    wide = pl.BlockSpec((d, CHUNK), lambda c, t: (0, c))
    tall = pl.BlockSpec((CHUNK, d), lambda c, t: (c, 0))
    tile = pl.BlockSpec((TILE, CHUNK), lambda c, t: (jnp.minimum(t, tiles - 1), c))
    shape = jax.ShapeDtypeStruct
    out = pl.pallas_call(
        functools.partial(lower_kernel, side, splits, chunks, tiles),
        grid=(chunks, tiles + 1),
        out_shape=[shape((ff, d), BF16), shape((tokens, d), BF16), shape((tokens, ff), BF16), shape((tokens, ff), BF16)]
        + [shape(block_shape(s, *t.shape[1:]), BF16) for s, t in zip(splits, terms)],
        in_specs=[whole, whole, tile, tile, wide, wide, tall] + [ANY] * n,
        out_specs=[tall, ANY, tile, tile]
        + [pl.BlockSpec(block_shape(s, *t.shape[1:]), lambda c, t: (0, 0)) for s, t in zip(splits, terms)],
        scratch_shapes=[
            pltpu.VMEM((tokens, d), F32),
            pltpu.VMEM((tokens, CHUNK), BF16),
            pltpu.VMEM((tokens, d), BF16),
            pltpu.SemaphoreType.DMA(()),
        ]
        + [b for s, t in zip(splits, terms) for b in Scatter.scratch(side, s, *t.shape[1:])]
        + [pltpu.SemaphoreType.DMA((n, Scatter.SEMS)), pltpu.SemaphoreType.DMA((n, Scatter.SEMS))],
        compiler_params=pltpu.CompilerParams(
            collective_id=collective_id,
            has_side_effects=True,
            vmem_limit_bytes=67043328,
            dimension_semantics=("arbitrary", "arbitrary"),
        ),
        name="lower",
    )(h, g, *kept, *weights, *terms)
    return out[0], out[1], out[2:4], out[4:]


PIECES = 4


def wide_kernel(side, at_ref, dg_ref, du_ref, down_ref, *refs):
    outs, terms, bufs, (send, recv) = refs[:5], refs[5:9], refs[9:49], refs[49:]
    slot = pl.program_id(0)
    place = Place(side)
    sources, splits = (down_ref, *terms), ("rows",) + ("columns",) * 4
    events = [(0, functools.partial(greet, place))]
    for i in range(5):
        s = Scatter(
            place, splits[i], sources[i], outs[i], bufs[8 * i : 8 * i + 8], send.at[i], recv.at[i], near=i > 0
        )
        times = (0, 4, 5, 6, 7, 8, 11, 17, 22, 26) if i == 0 else (0, 2, 3, 4, 5, 6, 9, 14, 18, 22)
        events += s.timed(2 * PIECES * i, times)
    run_at(slot, 8 * PIECES + 1, events)
    chips, height, _ = terms[0].shape
    some = chips // PIECES
    for i in range(4):

        @pl.when(slot // (2 * PIECES) == i)
        def _(i=i):
            q = slot // 2 % PIECES
            width = terms[i].shape[-1] // 2
            columns = pl.ds(pl.multiple_of(slot % 2 * width, 128), width)
            rows = pl.ds(pl.multiple_of(q * some * height, some * height), some * height)
            got = dot(at_ref[rows, :], (dg_ref, du_ref)[i // 2][:, columns])
            terms[i][pl.ds(q * some, some), :, columns] = got.reshape(some, height, got.shape[-1]).astype(BF16)


def wide_grads(side, chips, at, hidden, down, collective_id):
    d, tokens = at.shape
    ff = hidden[0].shape[1]
    half, height = ff // 2, d // chips
    shapes = [block_shape("rows", *down.shape[1:])] + [block_shape("columns", height, half)] * 4
    splits, sizes = ("rows",) + ("columns",) * 4, [down.shape[1:]] + [(height, half)] * 4
    return pl.pallas_call(
        functools.partial(wide_kernel, side),
        grid=(8 * PIECES + 1,),
        out_shape=[jax.ShapeDtypeStruct(s, BF16) for s in shapes],
        in_specs=[
            pl.BlockSpec((d, tokens), lambda s: (0, 0), pipeline_mode=pl.Buffered(1)),
            pl.BlockSpec((tokens, half), lambda s: (0, jnp.minimum(s // (2 * PIECES), 1))),
            pl.BlockSpec((tokens, half), lambda s: (0, jnp.clip(s // (2 * PIECES) - 2, 0, 1))),
            ANY,
        ],
        out_specs=[pl.BlockSpec(s, lambda i: (0, 0)) for s in shapes],
        scratch_shapes=[pltpu.VMEM((chips, height, half), BF16)] * 4
        + [b for s, z in zip(splits, sizes) for b in Scatter.scratch(side, s, *z)]
        + [pltpu.SemaphoreType.DMA((5, Scatter.SEMS)), pltpu.SemaphoreType.DMA((5, Scatter.SEMS))],
        compiler_params=pltpu.CompilerParams(
            collective_id=collective_id,
            has_side_effects=True,
            vmem_limit_bytes=67043328,
            dimension_semantics=("arbitrary",),
        ),
        name="wide_grads",
    )(at, *hidden, down)


def solution(mesh):
    n = mesh.shape["dp"]
    chips = n // 2
    side = math.isqrt(chips)
    splits = ("columns", "columns", "rows")
    swap = [(i, i ^ 1) for i in range(n)]

    def step(x, dy, w_gate, w_up, w_down):
        x, dy = x[0], dy[0]
        layers, d_own, ff = w_gate.shape
        f_own, d = w_down.shape[1:]
        core = lax.axis_index("dp") % 2

        both = jnp.stack([w_gate, w_up])
        other = lax.ppermute(both, "dp", swap)
        both = jnp.where(core == 0, jnp.concatenate([both, other], 2), jnp.concatenate([other, both], 2))
        downs = jnp.pad(w_down, ((0, 0), (0, f_own), (0, 0)))
        downs = jnp.where(core == 0, downs, jnp.roll(downs, f_own, 1))
        blocks = [[both[0, l : l + 1], both[1, l : l + 1], downs[l : l + 1]] for l in range(layers)]

        def flat(full):
            return [f.reshape(-1, f.shape[-1]) for f in full]

        weights = [flat(gather(side, chips, splits, blocks[0], 1))]
        hs, kept = [x], []
        for l in range(layers):
            if l < layers - 1:
                h, saved, full = forward(side, chips, splits, hs[l], weights[l], blocks[l + 1], 3)
                hs.append(h)
                kept.append(saved)
                weights.append(flat(full))

        def tall(t):
            return t.reshape(chips, -1, t.shape[-1])

        def whole(mine):
            lower, upper = mine[:, :d_own], mine[:, d_own:]
            got = lax.ppermute(jnp.where(core == 0, upper, lower), "dp", swap)
            return jnp.where(core == 0, jnp.concatenate([lower, got], -1), jnp.concatenate([got, upper], -1))

        grads, g = top(hs[-1], dy, weights[-1])
        by_gate, by_up, by_down = [], [], []
        terms = [tall(t) for t in grads]
        for l in reversed(range(layers - 1)):
            down, g, hidden, done = lower(side, splits, kept[l][:2], hs[l], g, weights[l], terms, 4)
            both = whole(jnp.stack(done[:2]))
            by_gate.append(both[0])
            by_up.append(both[1])
            by_down.append(done[2])
            done = wide_grads(side, chips, kept[l][2], hidden, tall(down), 2)
            four = whole(jnp.stack(done[1:]))
            by_gate.append(jnp.concatenate([four[0], four[1]], -1))
            by_up.append(jnp.concatenate([four[2], four[3]], -1))
            by_down.append(done[0])
        return g[None], *(jnp.stack(t[::-1]) for t in (by_gate, by_up, by_down))

    wspec = P(None, "dp", None)
    out = P("rep", "dp", None)
    rows = P(("rep", "dp"), None, None)
    return jax.shard_map(
        step, mesh=mesh, in_specs=(rows, rows, wspec, wspec, wspec), out_specs=(rows, out, out, out), check_vma=False
    )
```
